512 devices in a mesh: tm: 8 (over y_hi, x), height: 64 (over y_lo, z, core).
Axes of the slice: x: 4, y: 8 (y_hi: 2, y_lo: 4; y = y_hi * 4 + y_lo), z: 8, core: 2. Of those that a mesh axis runs over, the one named last changes fastest.
Arguments:
- pixels: bfloat16 [16, 3, 512, 1024], P('tm', None, 'height'), may hold values from -6 to 6
- conv_weight: bfloat16 [3, 3, 3, 48, 128], replicated, may hold values from -0.15625 to 0.15625
- conv_bias: float32 [128], replicated, may hold values from -3 to 3
- down_weight: bfloat16 [2, 2, 128, 256], replicated, may hold values from -0.25 to 0.25
- down_bias: float32 [256], replicated, may hold values from -3 to 3
- cotangent: bfloat16 [16, 64, 128, 256], P('tm', 'height'), may hold values from -6 to 6
Outputs:
- features: bfloat16 [16, 64, 128, 256], P('tm', 'height')
- grad_conv: float32 [3, 3, 3, 48, 128], replicated
- grad_conv_bias: float32 [128], replicated
- grad_down: float32 [2, 2, 128, 256], replicated
- grad_down_bias: float32 [256], replicated
- grad_pixels: float32 [16, 3, 512, 1024], P('tm', None, 'height')
The draws below stay inside these ranges and needn't reach their ends.
All inputs are finite; a program needn't handle non-finite values.
Results may differ from the reference program's by a relative error of at most 0.012.
Values may be sent and summed in bfloat16 or wider, within the bound.
A program may use at most 64 MiB of HBM per device.

```python
import math
import jax
import jax.numpy as jnp
import numpy as np
from jax import lax

COLS = 256
COEFFS = 48
C1 = 128
C2 = 256
FRAMES = 16
ROWS = 128
HEIGHT_PX = 512
WIDTH_PX = 1024
HALF_ROWS = 64
HALF_COLS = 128


def levels(stream_key, shape, split, low, largest):
    def one(position, shards_of):
        draws = jax.random.uniform(jax.random.fold_in(jax.random.fold_in(stream_key, 6), position), (shards_of,), jnp.float32, low / len(split), largest / len(split))
        return jnp.repeat(jnp.exp(draws), shape[position] // shards_of).reshape((-1,) + (1,) * (len(shape) - position - 1))

    level = one(*split[0])
    for cut in split[1:]:
        level = level * one(*cut)
    return level


def normal_values(stream_key, shape, spread, most, cuts=(), dtype=jnp.bfloat16):
    values = spread * jax.random.normal(stream_key, shape, jnp.float32)
    if cuts:
        values = values * levels(stream_key, shape, cuts, -0.22, 0.18)
    return jnp.clip(values, -most, most).astype(dtype)


def setup_inputs(seed: int = 0) -> dict:
    splits = jax.random.split(jax.random.key(seed), 7)
    return {
        "pixels": normal_values(splits[0], (FRAMES, 3, HEIGHT_PX, WIDTH_PX), 1.0, 6.0, ((0, 8), (2, 64))),
        "conv_weight": normal_values(splits[1], (3, 3, 3, COEFFS, C1), (27 * COEFFS) ** -0.5, 0.15625),
        "conv_bias": normal_values(splits[2], (C1,), 0.5, 3.0, (), jnp.float32),
        "down_weight": normal_values(splits[3], (2, 2, C1, C2), (4 * C1) ** -0.5, 0.25),
        "down_bias": normal_values(splits[4], (C2,), 0.5, 3.0, (), jnp.float32),
        "cotangent": normal_values(splits[5], (FRAMES, HALF_ROWS, HALF_COLS, C2), 1.0, 6.0, ((0, 8), (1, 64))),
    }


haar_matrix = np.kron(np.array([[1.0, 1.0], [1.0, -1.0]]), np.array([[1.0, 1.0], [1.0, -1.0]])) * 0.5

def analyse(pixels):
    frame_count, colors, height_px, width_px = pixels.shape
    table = jnp.asarray(haar_matrix, jnp.float32)
    blocks = pixels.astype(jnp.float32).reshape(frame_count, colors, height_px // 4, 4, width_px // 4, 4)
    result = jnp.einsum('fkrucv,iu,jv->fkijrc', blocks, table, table)
    return result.reshape(frame_count, colors * 16, height_px // 4, width_px // 4)

def synthesise(dcoeffs):
    frame_count, channels, height_cells, width_cells = dcoeffs.shape
    table = jnp.asarray(haar_matrix, jnp.float32)
    parts = dcoeffs.reshape(frame_count, channels // 16, 4, 4, height_cells, width_cells)
    result = jnp.einsum('fkijrc,iu,jv->fkrucv', parts, table, table)
    return result.reshape(frame_count, channels // 16, height_cells * 4, width_cells * 4)

def reference(pixels, conv_weight, conv_bias, down_weight, down_bias, cotangent):
    coeffs = analyse(pixels).astype(jnp.bfloat16)
    frame_count, channels, height_cells, width_cells = coeffs.shape
    outer = conv_weight.shape[-1]
    extended = jnp.pad(coeffs, ((2, 0), (0, 0), (1, 1), (1, 1))).astype(jnp.float32)
    weight32 = conv_weight.astype(jnp.float32)
    pre = jnp.zeros((frame_count, height_cells, width_cells, outer), jnp.float32) + conv_bias
    windows = []
    for tap_time in range(3):
        for tap_row in range(3):
            for tap_col in range(3):
                window = extended[tap_time:tap_time + frame_count, :, tap_row:tap_row + height_cells, tap_col:tap_col + width_cells]
                windows.append((tap_time, tap_row, tap_col))
                pre = pre + jnp.einsum('fkrc,ko->frco', window, weight32[tap_time, tap_row, tap_col])
    act = jax.nn.silu(pre).astype(jnp.bfloat16)
    down32 = down_weight.astype(jnp.float32)
    grouped = act.astype(jnp.float32).reshape(frame_count, height_cells // 2, 2, width_cells // 2, 2, outer)
    features = (jnp.einsum('fqupvk,uvko->fqpo', grouped, down32) + down_bias).astype(jnp.bfloat16)
    cot32 = cotangent.astype(jnp.float32)
    dact = jnp.einsum('fqpo,uvko->fqupvk', cot32, down32).reshape(frame_count, height_cells, width_cells, outer)
    sig = jax.nn.sigmoid(pre)
    slope = (dact * sig * (1.0 + pre * (1.0 - sig))).astype(jnp.bfloat16)
    slope32 = slope.astype(jnp.float32)
    scale = 1.0 / math.sqrt(FRAMES * ROWS * COLS)
    grad_down = scale * jnp.einsum('fqupvk,fqpo->uvko', grouped, cot32)
    grad_down_bias = scale * lax.optimization_barrier(jnp.sum(cot32, axis=(0, 1, 2)))
    pieces = []
    for tap_time, tap_row, tap_col in windows:
        window = extended[tap_time:tap_time + frame_count, :, tap_row:tap_row + height_cells, tap_col:tap_col + width_cells]
        pieces.append(jnp.einsum('fkrc,frco->ko', window, slope32))
    grad_conv = scale * jnp.stack(pieces).reshape(3, 3, 3, channels, outer)
    grad_conv_bias = scale * lax.optimization_barrier(jnp.sum(slope32, axis=(0, 1, 2)))
    later = jnp.pad(slope32, ((0, 2), (1, 1), (1, 1), (0, 0)))
    dcoeffs = jnp.zeros((frame_count, channels, height_cells, width_cells), jnp.float32)
    for tap_time, tap_row, tap_col in windows:
        window = later[2 - tap_time:2 - tap_time + frame_count, 2 - tap_row:2 - tap_row + height_cells, 2 - tap_col:2 - tap_col + width_cells]
        dcoeffs = dcoeffs + jnp.einsum('frco,ko->fkrc', window, weight32[tap_time, tap_row, tap_col])
    grad_pixels = synthesise(dcoeffs)
    return (features, grad_conv, grad_conv_bias, grad_down, grad_down_bias, grad_pixels)
```

```python
import functools
import math

import jax
import jax.numpy as jnp
from jax import lax
from jax.experimental import pallas as pl
from jax.experimental.pallas import tpu as pltpu
from jax.sharding import PartitionSpec as P

MESH = pl.DeviceIdType.MESH
F32 = jnp.float32
BF16 = jnp.bfloat16

FACTORS = {"y_hi": 2, "x": 4, "y_lo": 4, "z": 8}

TAPS = 27 * 48
BAND = 9 * 48
CELL = 3 * 48
GRAD_ROWS = TAPS + 1024 + 24


def dot(a, b, contract):
    return lax.dot_general(a, b, (contract, ((), ())), preferred_element_type=F32)


NN = ((1,), (0,))
NT = ((1,), (1,))
TN = ((0,), (0,))


def to_right(value):
    even, odd = value[:, :128], value[:, 128:]
    lane = lax.broadcasted_iota(jnp.int32, even.shape, 1)
    moved = jnp.where(lane == 127, 0.0, pltpu.roll(even, 127, axis=1))
    return odd, moved


def to_left(value):
    even, odd = value[:, :128], value[:, 128:]
    lane = lax.broadcasted_iota(jnp.int32, even.shape, 1)
    moved = jnp.where(lane == 0, 0.0, pltpu.roll(odd, 1, axis=1))
    return moved, even


def butterfly(parts):
    p0, p1, p2, p3 = parts
    a, b, c, d = p0 + p1, p0 - p1, p2 + p3, p2 - p3
    return a + c, b + d, a - c, b - d


def main_kernel(
    fac, m,
    px, w, cb_ref, dw, db_ref, cot,
    feat, gp, gath,
    wt, haar, y32, c32, cext, shifted, acc, dact, act, slope,
    grads, csend, crecv, p1, xsend, xrecv, p2, ysend, yrecv, zbuf,
    esend, erecv, e32, tsend, trecv, ef,
    hs_sem, hr_sem, es_sem, er_sem,
    cs_sem, cr_sem, xs_sem, xr_sem, ys_sem, yr_sem, zs_sem, zr_sem,
    ay_s, ay_r, ax_s, ax_r, ac_s, ac_r,
):
    X, Y0, Z = fac["x"], fac["y_lo"], fac["z"]
    NY = fac["y_hi"] * Y0
    T, H = fac["y_hi"] * X, Y0 * Z * 2
    tm, h = lax.axis_index("tm"), lax.axis_index("height")
    core = lax.rem(h, 2)
    z = lax.rem(lax.div(h, 2), Z)
    y_lo = lax.div(h, 2 * Z)
    x = lax.rem(tm, X)
    y = lax.div(tm, X) * Y0 + y_lo
    other = 1 - core

    def dev(x_, y_, z_, c_):
        return (lax.div(y_, Y0) * X + x_, lax.rem(y_, Y0) * (2 * Z) + z_ * 2 + c_)

    partner = dev(x, y, z, other)
    xs = [lax.rem(x + d, X) for d in range(1, X)]
    ys = [lax.rem(y + d, NY) for d in range(1, NY)]
    zs = [lax.rem(z + d, Z) for d in range(1, Z)]
    xdev = [dev(v, y, z, core) for v in xs]
    ydev = [dev(x, v, z, core) for v in ys]
    zdev = [dev(x, y, v, core) for v in zs]
    up, down = (tm, lax.rem(h + H - 1, H)), (tm, lax.rem(h + 1, H))
    prev, nxt = (lax.rem(tm + T - 1, T), h), (lax.rem(tm + 1, T), h)
    has_up, has_down, has_prev, has_next = h > 0, h < H - 1, tm > 0, tm < T - 1

    barrier = pltpu.get_barrier_semaphore()
    for peer in [partner] + xdev + ydev + zdev:
        pl.semaphore_signal(barrier, inc=1, device_id=peer, device_id_type=MESH)
    for there, peer in ((has_up, up), (has_down, down), (has_prev, prev), (has_next, nxt)):

        @pl.when(there)
        def _(peer=peer):
            pl.semaphore_signal(barrier, inc=1, device_id=peer, device_id_type=MESH)

    def remote(src, dst, send, recv, peer):
        return pltpu.make_async_remote_copy(
            src_ref=src, dst_ref=dst, send_sem=send, recv_sem=recv,
            device_id=peer, device_id_type=MESH,
        )

    for block in range(4):
        row = lax.broadcasted_iota(jnp.int32, (256, 256), 0) + 256 * block
        col = lax.broadcasted_iota(jnp.int32, (256, 256), 1)
        hit = (row >> 3 == (col & 127)) & (((row >> 2) & 1) == (col >> 7))
        base = jnp.where(hit, 0.25, 0.0)
        low = (1 - 2 * (row & 1)).astype(F32)
        high = (1 - (row & 2)).astype(F32)
        for j, value in enumerate((base, base * low, base * high, base * low * high)):
            haar[256 * block : 256 * (block + 1), 256 * j : 256 * (j + 1)] = value.astype(BF16)

    stacked = jnp.concatenate(
        [px[f, k].astype(F32) for k in range(3) for f in range(2)], axis=0
    ).astype(BF16)
    value = dot(stacked, haar[...], NN)
    for n in range(8):
        y32[n] = value[:, 128 * n : 128 * (n + 1)]
    for k in range(3):
        for n in range(8):
            rows = butterfly([y32[n, pl.ds(16 * k + u, 4, stride=4), :] for u in range(4)])
            for i in range(4):
                at = 16 * k + 4 * i + n // 2
                c32[n % 2, pl.ds(at, 4, stride=48), :] = rows[i]
    for f in range(2):
        for r in range(2):
            at = (2 * f + r) * 48
            for e in range(2):
                cext[2 + f, 1 + r, :, 128 * e : 128 * (e + 1)] = c32[e, at : at + 48, :].astype(BF16)

    expected = (
        1 + (X - 1) + (NY - 1) + (Z - 1)
        + has_up.astype(jnp.int32) + has_down.astype(jnp.int32)
        + has_prev.astype(jnp.int32) + has_next.astype(jnp.int32)
    )
    pl.semaphore_wait(barrier, expected)

    to_next = remote(cext.at[2:4, 1:3], cext.at[0:2, 1:3], hs_sem.at[0], hr_sem.at[0], nxt)
    own_down = remote(cext.at[2:4, 2], cext.at[2:4, 0], hs_sem.at[1], hr_sem.at[1], down)
    own_up = remote(cext.at[2:4, 1], cext.at[2:4, 3], hs_sem.at[2], hr_sem.at[2], up)
    far_down = remote(cext.at[0:2, 2], cext.at[0:2, 0], hs_sem.at[3], hr_sem.at[3], down)
    far_up = remote(cext.at[0:2, 1], cext.at[0:2, 3], hs_sem.at[4], hr_sem.at[4], up)

    @pl.when(has_next)
    def _():
        to_next.start()

    @pl.when(has_down)
    def _():
        own_down.start()

    @pl.when(has_up)
    def _():
        own_up.start()

    @pl.when(h == 0)
    def _():
        for f in range(4):
            cext[f, 0] = jnp.zeros((48, 256), BF16)

    @pl.when(h == H - 1)
    def _():
        for f in range(4):
            cext[f, 3] = jnp.zeros((48, 256), BF16)

    @pl.when(tm == 0)
    def _():
        for f in range(2):
            for r in range(4):
                cext[f, r] = jnp.zeros((48, 256), BF16)

    def shift(f, r):
        block = cext[f, r]
        wide = block.astype(F32)
        left, right = to_left(wide), to_right(wide)
        shifted[f, r, 0:48, 0:128] = left[0].astype(BF16)
        shifted[f, r, 0:48, 128:256] = left[1].astype(BF16)
        shifted[f, r, 48:96, :] = block
        shifted[f, r, 96:144, 0:128] = right[0].astype(BF16)
        shifted[f, r, 96:144, 128:256] = right[1].astype(BF16)

    for a in range(3):
        wt[a] = w[BAND * a : BAND * (a + 1), :].astype(F32).T.astype(BF16)
    for f in range(2):
        for r in range(2):
            for e in range(2):
                at = 128 * (2 * r + e)
                dact[f, r, :, 128 * e : 128 * (e + 1)] = dot(dw[at : at + 128, :], cot[f], NT)
    for f in range(2):
        for r in range(2):
            shift(2 + f, 1 + r)

    def taps(f, r):
        return shifted[f, r : r + 3].reshape(BAND, 256)

    @pl.when(has_up)
    def _():
        own_down.wait_recv()

    @pl.when(has_down)
    def _():
        own_up.wait_recv()

    for f in range(2):
        shift(2 + f, 0)
        shift(2 + f, 3)
    for r in range(2):
        acc[0, r] = dot(wt[2], taps(2, r), NN)
        acc[1, r] = dot(wt[1], taps(2, r), NN) + dot(wt[2], taps(3, r), NN)

    @pl.when(has_prev)
    def _():
        to_next.wait_recv()

        @pl.when(has_down)
        def _():
            far_down.start()

        @pl.when(has_up)
        def _():
            far_up.start()

    for f in range(2):
        for r in range(2):
            shift(f, 1 + r)

    @pl.when(has_prev & has_up)
    def _():
        far_down.wait_recv()

    @pl.when(has_prev & has_down)
    def _():
        far_up.wait_recv()

    for f in range(2):
        shift(f, 0)
        shift(f, 3)

    bias = cb_ref[...]
    for f in range(2):
        for r in range(2):
            pre = acc[f, r] + bias
            if f == 0:
                pre = pre + (dot(wt[0], taps(0, r), NN) + dot(wt[1], taps(1, r), NN))
            else:
                pre = pre + dot(wt[0], taps(1, r), NN)
            sig = jax.nn.sigmoid(pre)
            act[f, r] = (pre * sig).astype(BF16)
            slope[f, r] = (dact[f, r] * sig * (1.0 + pre * (1.0 - sig))).astype(BF16)

    half = X * NY * m

    def put(at, value):
        count = value.shape[0]
        first = max(0, min(count, half - at))
        if first:
            grads[0, at : at + first, :] = value[:first]
        if first < count:
            start = at + first - half
            grads[1, start : start + count - first, :] = value[first:]

    for a in range(3):
        total = None
        for f in range(2):
            for r in range(2):
                part = dot(taps(f + a, r), slope[f, r], NT)
                total = part if total is None else total + part
        put(BAND * a, total)
    for u in range(2):
        for v in range(2):
            total = dot(act[0, u, :, 128 * v : 128 * (v + 1)], cot[0], NN) + dot(
                act[1, u, :, 128 * v : 128 * (v + 1)], cot[1], NN
            )
            at = TAPS + 128 * (2 * u + v)
            put(at, total[:, :128])
            put(at + 512, total[:, 128:])
    ones = jnp.ones((8, 256), BF16)
    total = None
    for f in range(2):
        for r in range(2):
            part = dot(ones, slope[f, r], NT)
            total = part if total is None else total + part
    put(TAPS + 1024, total)
    total = dot(ones[:, :128], cot[0], NN) + dot(ones[:, :128], cot[1], NN)
    put(TAPS + 1032, total[:, :128])
    put(TAPS + 1040, total[:, 128:])
    if GRAD_ROWS < 2 * half:
        put(GRAD_ROWS, jnp.zeros((2 * half - GRAD_ROWS, 128), F32))

    csend[...] = grads[other].reshape(X, NY, m, 128).astype(BF16)
    to_partner = remote(csend, crecv, cs_sem.at[0], cr_sem.at[0], partner)
    to_partner.start()

    for f in range(2):
        total = None
        for u in range(2):
            for v in range(2):
                at = 128 * (2 * u + v)
                part = dot(act[f, u, :, 128 * v : 128 * (v + 1)], dw[at : at + 128, :], TN)
                total = part if total is None else total + part
        feat[f] = (total + db_ref[...]).astype(BF16)

    to_partner.wait_recv()
    total = grads[core].reshape(X, NY, m, 128) + crecv[...].astype(F32)
    p1[...] = total
    xsend[...] = total.astype(BF16)
    to_x = [
        remote(xsend.at[v], xrecv.at[i], xs_sem.at[i], xr_sem.at[i], xdev[i])
        for i, v in enumerate(xs)
    ]
    for c in to_x:
        c.start()

    def dcoeffs(fe, re):
        total = None
        for f in range(2):
            for r in range(2):
                a, b = fe - f, re - r
                if 0 <= a < 3 and 0 <= b < 3:
                    at = CELL * (3 * a + b)
                    part = dot(w[at : at + CELL, :], slope[f, r], NN)
                    total = part if total is None else total + part
        right = to_right(total[0:48])
        left = to_left(total[96:144])
        mid = total[48:96]
        return mid[:, :128] + right[0] + left[0], mid[:, 128:] + right[1] + left[1]

    for fe in range(4):
        for i, re in enumerate((0, 3)):
            even, odd = dcoeffs(fe, re)
            esend[i, fe, :, 0:128] = even.astype(BF16)
            esend[i, fe, :, 128:256] = odd.astype(BF16)
    e_up = remote(esend.at[0], erecv.at[0], es_sem.at[0], er_sem.at[0], up)
    e_down = remote(esend.at[1], erecv.at[1], es_sem.at[1], er_sem.at[1], down)

    @pl.when(has_up)
    def _():
        e_up.start()

    @pl.when(has_down)
    def _():
        e_down.start()

    for fe in range(4):
        for re in range(2):
            even, odd = dcoeffs(fe, re + 1)
            e32[fe, re, :, 0:128] = even
            e32[fe, re, :, 128:256] = odd

    for c in to_x:
        c.wait_recv()
    total = p1[x]
    for i in range(X - 1):
        total = total + xrecv[i].astype(F32)
    p2[...] = total
    ysend[...] = total.astype(BF16)
    to_y = [
        remote(ysend.at[v], yrecv.at[i], ys_sem.at[i], yr_sem.at[i], ydev[i])
        for i, v in enumerate(ys)
    ]
    for c in to_y:
        c.start()

    @pl.when(has_down)
    def _():
        e_up.wait_recv()
        for fe in range(4):
            e32[fe, 1] = e32[fe, 1] + erecv[0, fe].astype(F32)

    @pl.when(has_up)
    def _():
        e_down.wait_recv()
        for fe in range(4):
            e32[fe, 0] = e32[fe, 0] + erecv[1, fe].astype(F32)

    for fe in range(2):
        for re in range(2):
            tsend[fe, re] = e32[fe, re].astype(BF16)

    for c in to_y:
        c.wait_recv()
    total = p2[y]
    for i in range(NY - 1):
        total = total + yrecv[i].astype(F32)
    zbuf[z] = total.astype(BF16)
    to_z = [
        remote(zbuf.at[z], zbuf.at[z], zs_sem.at[i], zr_sem.at[i], zdev[i]) for i in range(Z - 1)
    ]
    for c in to_z:
        c.start()

    to_prev = remote(tsend, trecv, es_sem.at[2], er_sem.at[2], prev)

    @pl.when(has_prev)
    def _():
        to_prev.start()

    for c in to_z:
        c.wait_recv()
    total = zbuf[0].astype(F32)
    for i in range(1, Z):
        total = total + zbuf[i].astype(F32)
    gath[core, x, y] = total.astype(BF16)

    all_y = [
        remote(gath.at[core, x, y], gath.at[core, x, y], ay_s.at[i], ay_r.at[i], ydev[i])
        for i in range(NY - 1)
    ]
    for c in all_y:
        c.start()

    def synthesis():
        for f in range(2):
            for r in range(2):
                at = (2 * f + r) * 48
                for e in range(2):
                    ef[e, at : at + 48, :] = e32[2 + f, r, :, 128 * e : 128 * (e + 1)]

        @pl.when(has_next)
        def _():
            to_prev.wait_recv()
            for f in range(2):
                for r in range(2):
                    at = (2 * f + r) * 48
                    for e in range(2):
                        more = trecv[f, r, :, 128 * e : 128 * (e + 1)].astype(F32)
                        ef[e, at : at + 48, :] = ef[e, at : at + 48, :] + more

        for k in range(3):
            for n in range(8):
                rows = butterfly(
                    [ef[n % 2, pl.ds(16 * k + 4 * i + n // 2, 4, stride=48), :] for i in range(4)]
                )
                for u in range(4):
                    y32[n, pl.ds(16 * k + u, 4, stride=4), :] = rows[u]
        value = jnp.concatenate([y32[n] for n in range(8)], axis=1)
        high = value.astype(BF16)
        low = (value - high.astype(F32)).astype(BF16)
        both = dot(jnp.concatenate([high, low], axis=0), haar[...], NT)
        result = both[:48] + both[48:]
        for k in range(3):
            for f in range(2):
                at = 16 * k + 8 * f
                gp[f, k] = result[at : at + 8]

    for c in all_y:
        c.wait_recv()
    all_x = [
        remote(gath.at[core, x], gath.at[core, x], ax_s.at[i], ax_r.at[i], xdev[i])
        for i in range(X - 1)
    ]
    for c in all_x:
        c.start()
    back = [x] + [lax.rem(x + X - d, X) for d in range(1, X)]
    all_c = [
        remote(gath.at[core, v], gath.at[core, v], ac_s.at[i], ac_r.at[i], partner)
        for i, v in enumerate(back)
    ]
    all_c[0].start()
    synthesis()
    for i in range(1, X):
        all_x[i - 1].wait_recv()
        all_c[i].start()
    for i in range(X):
        all_c[i].wait_recv()

    @pl.when(has_next)
    def _():
        to_next.wait_send()

    @pl.when(has_down)
    def _():
        own_down.wait_send()
        e_down.wait_send()

    @pl.when(has_up)
    def _():
        own_up.wait_send()
        e_up.wait_send()

    @pl.when(has_prev & has_down)
    def _():
        far_down.wait_send()

    @pl.when(has_prev & has_up)
    def _():
        far_up.wait_send()

    @pl.when(has_prev)
    def _():
        to_prev.wait_send()

    to_partner.wait_send()
    for c in to_x + to_y + to_z + all_y + all_x + all_c:
        c.wait_send()


def finish_kernel(scale, g_ref, gc_ref, gcb_ref, gd_ref, gdb_ref):
    value = g_ref[...].astype(F32)
    value = value.reshape(-1, 128) * scale
    gc_ref[...] = value[:TAPS]
    gd_ref[:, 0:128] = value[TAPS : TAPS + 512]
    gd_ref[:, 128:256] = value[TAPS + 512 : TAPS + 1024]
    gcb_ref[...] = value[TAPS + 1024 : TAPS + 1025]
    gdb_ref[:, 0:128] = value[TAPS + 1032 : TAPS + 1033]
    gdb_ref[:, 128:256] = value[TAPS + 1040 : TAPS + 1041]


def local(pixels, conv_weight, conv_bias, down_weight, down_bias, cotangent):
    fac = FACTORS
    X, Z = fac["x"], fac["z"]
    NY = fac["y_hi"] * fac["y_lo"]
    pieces = 2 * X * NY
    m = -(-GRAD_ROWS // (8 * pieces)) * 8
    vmem = pltpu.VMEM
    dma = pltpu.SemaphoreType.DMA
    inside = pl.BlockSpec(memory_space=vmem)
    scratch = [
        vmem((3, 128, BAND), BF16),
        vmem((1024, 1024), BF16),
        vmem((8, 48, 128), F32),
        vmem((2, 192, 128), F32),
        vmem((4, 4, 48, 256), BF16),
        vmem((4, 4, CELL, 256), BF16),
        vmem((2, 2, 128, 256), F32),
        vmem((2, 2, 128, 256), F32),
        vmem((2, 2, 128, 256), BF16),
        vmem((2, 2, 128, 256), BF16),
        vmem((2, X * NY * m, 128), F32),
        vmem((X, NY, m, 128), BF16),
        vmem((X, NY, m, 128), BF16),
        vmem((X, NY, m, 128), F32),
        vmem((X, NY, m, 128), BF16),
        vmem((X - 1, NY, m, 128), BF16),
        vmem((NY, m, 128), F32),
        vmem((NY, m, 128), BF16),
        vmem((NY - 1, m, 128), BF16),
        vmem((Z, m, 128), BF16),
        vmem((2, 4, 48, 256), BF16),
        vmem((2, 4, 48, 256), BF16),
        vmem((4, 2, 48, 256), F32),
        vmem((2, 2, 48, 256), BF16),
        vmem((2, 2, 48, 256), BF16),
        vmem((2, 192, 128), F32),
        dma((5,)), dma((5,)), dma((3,)), dma((3,)),
        dma((1,)), dma((1,)), dma((X - 1,)), dma((X - 1,)),
        dma((NY - 1,)), dma((NY - 1,)), dma((Z - 1,)), dma((Z - 1,)),
        dma((NY - 1,)), dma((NY - 1,)), dma((X - 1,)), dma((X - 1,)),
        dma((X,)), dma((X,)),
    ]
    features, grad_pixels, gathered = pl.pallas_call(
        functools.partial(main_kernel, fac, m),
        out_shape=(
            jax.ShapeDtypeStruct((2, 128, 256), BF16),
            jax.ShapeDtypeStruct((2, 3, 8, 1024), F32),
            jax.ShapeDtypeStruct((2, X, NY, m, 128), BF16),
        ),
        in_specs=[inside] * 6,
        out_specs=(inside,) * 3,
        scratch_shapes=scratch,
        compiler_params=pltpu.CompilerParams(
            collective_id=0, has_side_effects=True, vmem_limit_bytes=48 * 1024 * 1024
        ),
        name="front",
    )(
        pixels,
        conv_weight.reshape(TAPS, 128),
        conv_bias.reshape(128, 1),
        down_weight.reshape(512, 256),
        down_bias.reshape(1, 256),
        cotangent.reshape(2, 128, 256),
    )
    count = 2 * lax.axis_size("tm") * 2 * lax.axis_size("height") * 256
    grad_conv, grad_conv_bias, grad_down, grad_down_bias = pl.pallas_call(
        functools.partial(finish_kernel, 1.0 / math.sqrt(count)),
        out_shape=(
            jax.ShapeDtypeStruct((TAPS, 128), F32),
            jax.ShapeDtypeStruct((1, 128), F32),
            jax.ShapeDtypeStruct((512, 256), F32),
            jax.ShapeDtypeStruct((1, 256), F32),
        ),
        in_specs=[inside],
        out_specs=(inside,) * 4,
        compiler_params=pltpu.CompilerParams(vmem_limit_bytes=16 * 1024 * 1024),
        name="finish",
    )(gathered)
    return (
        features.reshape(2, 1, 128, 256),
        grad_conv.reshape(3, 3, 3, 48, 128),
        grad_conv_bias.reshape(128),
        grad_down.reshape(2, 2, 128, 256),
        grad_down_bias.reshape(256),
        grad_pixels,
    )


def solution(mesh):
    return jax.shard_map(
        local,
        mesh=mesh,
        in_specs=(P("tm", None, "height", None), P(), P(), P(), P(), P("tm", "height", None, None)),
        out_specs=(
            P("tm", "height", None, None),
            P(),
            P(),
            P(),
            P(),
            P("tm", None, "height", None),
        ),
        check_vma=False,
    )
```
